32 devices in a mesh: rows: 4 (over y, x), keys: 8 (over z, core).
Axes of the slice: x: 2, y: 2, z: 4, core: 2. Of those that a mesh axis runs over, the one named last changes fastest.
Arguments:
- pair_rep: bfloat16 [192, 384, 128], P('rows', 'keys'), may hold values from -6 to 6
- norm_gain: float32 [128], replicated, may hold values from 0.1 to 1.9
- w_query: bfloat16 [128, 128], replicated, may hold values from -0.5 to 0.5
- w_key: bfloat16 [128, 128], replicated, may hold values from -0.5 to 0.5
- w_value: bfloat16 [128, 128], replicated, may hold values from -0.5 to 0.5
- w_gate: bfloat16 [128, 128], replicated, may hold values from -0.5 to 0.5
- w_out: bfloat16 [128, 128], replicated, may hold values from -0.5 to 0.5
- pair_bias: bfloat16 [4, 384, 384], P(None, 'keys', 'rows'), may hold values from -12 to 300
Outputs:
- update: bfloat16 [192, 384, 128], P('rows', 'keys')
The draws below stay inside these ranges and needn't reach their ends.
All inputs are finite; a program needn't handle non-finite values.
Results may differ from the reference program's by a relative error of at most 0.025.
Values may be sent and summed in bfloat16 or wider, within the bound.
No kernel may reach another device: no remote copies, remote signals or barrier semaphores. Data moves between devices by JAX's collectives and lax.ppermute only.
A program may use at most 128 MiB of HBM per device.

```python
import jax
import jax.numpy as jnp
from jax import lax

CHANNELS = 128
HEADS = 4
HEAD_SIZE = 32
ROWS = 192
LENGTH = 384


def draw_pair_bias(key, part):
    shape = (HEADS, LENGTH, LENGTH)
    result = jnp.clip(2.0 * jax.random.normal(jax.random.fold_in(key, 6), shape, jnp.float32), -12.0, 12.0)
    return result.astype(jnp.bfloat16)


def block_scale(own_key, dims, split, low, high):
    level = 1.0
    for position, parts in split:
        draws = jax.random.uniform(jax.random.fold_in(jax.random.fold_in(own_key, 6), position), (parts,), jnp.float32, low / len(split), high / len(split))
        level = level * jnp.repeat(jnp.exp(draws), dims[position] // parts).reshape((-1,) + (1,) * (len(dims) - 1 - position))
    return level


def centred(stream_key, dims, deviation, limit, shards=(), held_as=jnp.bfloat16):
    factor_of = block_scale(stream_key, dims, shards, -0.22, 0.18) if shards else 1.0
    array = jax.random.normal(stream_key, dims, jnp.float32) * deviation * factor_of
    return jnp.minimum(jnp.maximum(array, -limit), limit).astype(held_as)


def setup_inputs(seed: int = 0) -> dict:
    splits = jax.random.split(jax.random.key(seed), 9)
    return {
        "pair_rep": centred(splits[0], (ROWS, LENGTH, CHANNELS), 1.0, 6.0, ((0, 4), (1, 8))),
        "norm_gain": jnp.clip(1.0 + 0.18 * jax.random.normal(splits[1], (CHANNELS,), jnp.float32), 0.1, 1.9),
        "w_query": centred(splits[2], (CHANNELS, HEADS * HEAD_SIZE), CHANNELS ** -0.5, 0.5),
        "w_key": centred(splits[3], (CHANNELS, HEADS * HEAD_SIZE), CHANNELS ** -0.5, 0.5),
        "w_value": centred(splits[4], (CHANNELS, HEADS * HEAD_SIZE), CHANNELS ** -0.5, 0.5),
        "w_gate": centred(splits[5], (CHANNELS, HEADS * HEAD_SIZE), CHANNELS ** -0.5, 0.5),
        "w_out": centred(splits[6], (HEADS * HEAD_SIZE, CHANNELS), (HEADS * HEAD_SIZE) ** -0.5, 0.5),
        "pair_bias": draw_pair_bias(jax.random.fold_in(splits[8], 71), 0),
    }


epsilon = 1e-05

def normalize(pair_rep, norm_gain):
    values = pair_rep.astype(jnp.float32)
    center = lax.optimization_barrier(jnp.mean(values, axis=-1, keepdims=True))
    spread = lax.optimization_barrier(jnp.mean(jnp.square(values - center), axis=-1, keepdims=True))
    return ((values - center) * lax.rsqrt(spread + epsilon) * norm_gain).astype(jnp.bfloat16)

def split_heads(tensor, head_count):
    return tensor.reshape(tensor.shape[:-1] + (head_count, tensor.shape[-1] // head_count))

def reference(pair_rep, norm_gain, w_query, w_key, w_value, w_gate, w_out, pair_bias):
    head_count = pair_bias.shape[0]
    inner_width = w_query.shape[1]
    normed = normalize(pair_rep, norm_gain)
    queries = (jnp.dot(normed, w_query, preferred_element_type=jnp.float32) * (inner_width // head_count) ** (-0.5)).astype(jnp.bfloat16)
    key_rows = jnp.dot(normed, w_key, preferred_element_type=jnp.float32).astype(jnp.bfloat16)
    value_rows = jnp.dot(normed, w_value, preferred_element_type=jnp.float32).astype(jnp.bfloat16)
    gates = jax.nn.sigmoid(jnp.dot(normed, w_gate, preferred_element_type=jnp.float32))
    bias_values = pair_bias.astype(jnp.float32)

    def one_row(arrays):
        query_row, key_row, value_row = arrays
        logits = jnp.einsum('jhd,khd->hjk', split_heads(query_row.astype(jnp.float32), head_count), split_heads(key_row.astype(jnp.float32), head_count), precision=lax.Precision.HIGHEST) + bias_values
        highest = lax.optimization_barrier(jnp.max(logits, axis=2, keepdims=True))
        powers = jnp.exp(logits - highest)
        totals = lax.optimization_barrier(jnp.sum(powers, axis=2))
        weights = lax.optimization_barrier(powers.astype(jnp.bfloat16)).astype(jnp.float32)
        summed = jnp.einsum('hjk,khd->jhd', weights, split_heads(value_row.astype(jnp.float32), head_count), precision=lax.Precision.HIGHEST)
        return (summed / jnp.transpose(totals)[..., None]).reshape(query_row.shape[0], inner_width)
    attended = lax.map(one_row, (queries, key_rows, value_rows))
    gated = (gates * attended).astype(jnp.bfloat16)
    return jnp.dot(gated, w_out, preferred_element_type=jnp.float32).astype(jnp.bfloat16)
```

```python
import functools

import jax
import jax.numpy as jnp
from jax import lax
from jax.experimental import pallas as pl
from jax.experimental.pallas import tpu as pltpu
from jax.sharding import PartitionSpec as P

epsilon = 1e-05
cores = 2
chunks = 1

f32 = jnp.float32
bf16 = jnp.bfloat16


def vmem(count):
    return [pl.BlockSpec(memory_space=pltpu.VMEM)] * count


def estimate(flops, size):
    return pl.CostEstimate(flops=flops, bytes_accessed=size, transcendentals=0)


def prepare_kernel(chips, x_ref, gain_ref, *out_refs):
    here = lax.axis_index("keys") // cores
    gain = gain_ref[...]
    for piece in range(chunks):
        for s in range(chips):
            values = x_ref[here ^ s, piece].astype(f32)
            center = jnp.mean(values, axis=-1, keepdims=True)
            moved = values - center
            spread = jnp.mean(jnp.square(moved), axis=-1, keepdims=True)
            normed = (moved * lax.rsqrt(spread + epsilon) * gain).astype(bf16)
            out_refs[piece * chips + s][...] = normed


def prepare(pair_rep, norm_gain, chips):
    rows, columns, channels = pair_rep.shape
    size = rows // chips // chunks
    view = pair_rep.reshape(chips, chunks, size, columns, channels)
    outs = pl.pallas_call(
        functools.partial(prepare_kernel, chips),
        out_shape=[jax.ShapeDtypeStruct((size, columns, channels), bf16)] * (chunks * chips),
        in_specs=vmem(2),
        out_specs=vmem(chunks * chips),
        name="prepare",
        cost_estimate=estimate(rows * columns * channels * 12, 4 * pair_rep.size),
    )(view, norm_gain.reshape(1, channels))
    return [outs[piece * chips : (piece + 1) * chips] for piece in range(chunks)]


def attend_kernel(chips, pieces, head_count, *refs):
    own, refs = refs[:chips], refs[chips:]
    other, refs = refs[:chips], refs[chips:]
    bias_refs, refs = refs[:pieces], refs[pieces:]
    wq_ref, wk_ref, wv_ref, wg_ref, wo_ref = refs[:5]
    out_refs, refs = refs[5 : 5 + chips], refs[5 + chips :]
    sources, tables, bias, queries, gates, keys, values = refs
    rows, columns, channels = own[0].shape
    width = wq_ref.shape[1]
    head_size = width // head_count
    count = chips * columns
    me = lax.axis_index("keys")
    here, core = me // cores, me % cores
    group = lax.axis_index("rows")
    for t in range(pieces):
        tables[group ^ t] = bias_refs[t][...]
    for s in range(chips):
        for h in range(head_count):
            bias[h, s * columns : (s + 1) * columns, :] = jnp.concatenate(
                [tables[p, s, h].astype(f32) for p in range(pieces)], axis=-1
            )
    for s in range(chips):
        chip = (here ^ s) * cores
        first = pl.multiple_of((chip + core) * columns, columns)
        second = pl.multiple_of((chip + 1 - core) * columns, columns)
        sources[:, pl.ds(first, columns), :] = own[s][...]
        sources[:, pl.ds(second, columns), :] = other[s][...]
    values[:, :, width:] = jnp.ones(values.shape[:2] + (width,), bf16)
    scale = head_size ** (-0.5)

    def project(row, carry):
        asking = jnp.concatenate([own[s][row] for s in range(chips)], axis=0)
        held = sources[row]
        queries[row] = (jnp.dot(asking, wq_ref[...], preferred_element_type=f32) * scale).astype(bf16)
        gates[row] = jax.nn.sigmoid(jnp.dot(asking, wg_ref[...], preferred_element_type=f32))
        keys[row] = jnp.dot(held, wk_ref[...], preferred_element_type=f32).astype(bf16)
        values[row, :, :width] = jnp.dot(held, wv_ref[...], preferred_element_type=f32).astype(bf16)
        return carry

    lax.fori_loop(0, rows, project, 0)
    lane_head = lax.broadcasted_iota(jnp.int32, (count, width), 1) // head_size

    def attend(row, carry):
        query = queries[row]
        key = keys[row]
        value = values[row]
        total = jnp.ones((count, width), f32)
        summed = jnp.zeros((count, width), f32)
        for h in range(head_count):
            chosen = lane_head == h
            logits = lax.dot_general(
                jnp.where(chosen, query, jnp.zeros_like(query)),
                key,
                (((1,), (1,)), ((), ())),
                preferred_element_type=f32,
            )
            logits = logits + bias[h]
            highest = jnp.max(logits, axis=-1, keepdims=True)
            powers = jnp.exp(logits - highest).astype(bf16)
            both = jnp.dot(powers, value, preferred_element_type=f32)
            summed = jnp.where(chosen, both[:, :width], summed)
            total = jnp.where(chosen, both[:, width:], total)
        gated = (gates[row] * (summed / total)).astype(bf16)
        update = jnp.dot(gated, wo_ref[...], preferred_element_type=f32).astype(bf16)
        for s in range(chips):
            out_refs[s][row] = update[s * columns : (s + 1) * columns]
        return carry

    lax.fori_loop(0, rows, attend, 0)


def attend(own, other, bias_pieces, weights, head_count):
    chips, pieces = len(own), len(bias_pieces)
    rows, columns, channels = own[0].shape
    width = weights[0].shape[1]
    count, length = chips * columns, chips * cores * columns
    flops = rows * (count * length * width * 6 + (2 * count + 2 * length) * channels * width * 2)
    return pl.pallas_call(
        functools.partial(attend_kernel, chips, pieces, head_count),
        out_shape=[jax.ShapeDtypeStruct((rows, columns, channels), bf16)] * chips,
        in_specs=vmem(2 * chips + pieces + 5),
        out_specs=vmem(chips),
        scratch_shapes=[
            pltpu.VMEM((rows, length, channels), bf16),
            pltpu.VMEM((pieces,) + bias_pieces[0].shape, bf16),
            pltpu.VMEM((head_count, count, length), f32),
            pltpu.VMEM((rows, count, width), bf16),
            pltpu.VMEM((rows, count, width), f32),
            pltpu.VMEM((rows, length, width), bf16),
            pltpu.VMEM((rows, length, 2 * width), bf16),
        ],
        name="attend",
        compiler_params=pltpu.CompilerParams(vmem_limit_bytes=60 * 2**20),
        cost_estimate=estimate(flops, 16 * rows * length * channels),
    )(*own, *other, *bias_pieces, *weights)


def place_kernel(chips, *refs):
    here = lax.axis_index("keys") // cores
    out_ref = refs[-1]
    for piece in range(chunks):
        for s in range(chips):
            out_ref[here ^ s, piece] = refs[piece * chips + s][...]


def place(blocks, chips):
    size, columns, channels = blocks[0].shape
    out = pl.pallas_call(
        functools.partial(place_kernel, chips),
        out_shape=jax.ShapeDtypeStruct((chips, chunks, size, columns, channels), bf16),
        in_specs=vmem(len(blocks)),
        out_specs=pl.BlockSpec(memory_space=pltpu.VMEM),
        name="place",
        cost_estimate=estimate(1000, 4 * size * columns * channels),
    )(*blocks)
    return out.reshape(chips * chunks * size, columns, channels)


def exchange_chips(block, s, chips):
    if s == 0:
        return block
    pairs = [(z * cores + c, (z ^ s) * cores + c) for z in range(chips) for c in range(cores)]
    return lax.ppermute(block, "keys", pairs)


def body(chips, groups, pair_rep, norm_gain, w_query, w_key, w_value, w_gate, w_out, pair_bias):
    head_count = pair_bias.shape[0]
    blocks = prepare(pair_rep, norm_gain, chips)
    mine = jnp.stack([exchange_chips(pair_bias, s, chips) for s in range(chips)])
    bias_pieces = [mine] + [
        lax.ppermute(mine, "rows", [(g, g ^ t) for g in range(groups)]) for t in range(1, groups)
    ]
    siblings = [(i, i ^ 1) for i in range(chips * cores)]
    weights = (w_query, w_key, w_value, w_gate, w_out)
    done = []
    for sent in blocks:
        own = [exchange_chips(sent[s], s, chips) for s in range(chips)]
        other = [lax.ppermute(block, "keys", siblings) for block in own]
        update = attend(own, other, bias_pieces, weights, head_count)
        done += [exchange_chips(update[s], s, chips) for s in range(chips)]
    return place(done, chips)


def solution(mesh):
    placed = (P("rows", "keys", None), P(), P(), P(), P(), P(), P(), P(None, "keys", "rows"))
    chips = mesh.shape["keys"] // cores
    return jax.shard_map(
        functools.partial(body, chips, mesh.shape["rows"]),
        mesh=mesh,
        in_specs=placed,
        out_specs=P("rows", "keys", None),
        check_vma=False,
    )
```

```python
import functools
import math

import jax
import jax.numpy as jnp
from jax import lax
from jax.experimental import pallas as pl
from jax.experimental.pallas import tpu as pltpu
from jax.sharding import PartitionSpec as P

epsilon = 1e-05
cores = 2
chunks = 1

f32 = jnp.float32
bf16 = jnp.bfloat16


def vmem(count):
    return [pl.BlockSpec(memory_space=pltpu.VMEM)] * count


def room(shapes, extra=4):
    size = sum(math.prod(s[:-1]) * max(s[-1], 128) * jnp.dtype(kind).itemsize for s, kind in shapes)
    return pltpu.CompilerParams(vmem_limit_bytes=min(size + extra * 2**20, 60 * 2**20))


def kinds(*arrays):
    return [(a.shape, a.dtype) for a in arrays]


def estimate(flops, size):
    return pl.CostEstimate(flops=flops, bytes_accessed=size, transcendentals=0)


def prepare_kernel(chips, x_ref, gain_ref, *out_refs):
    here = lax.axis_index("keys") // cores
    gain = gain_ref[...]
    for piece in range(chunks):
        for s in range(chips):
            values = x_ref[here ^ s, piece].astype(f32)
            center = jnp.mean(values, axis=-1, keepdims=True)
            moved = values - center
            spread = jnp.mean(jnp.square(moved), axis=-1, keepdims=True)
            normed = (moved * lax.rsqrt(spread + epsilon) * gain).astype(bf16)
            out_refs[piece * chips + s][...] = normed


def prepare(pair_rep, norm_gain, chips):
    rows, columns, channels = pair_rep.shape
    size = rows // chips // chunks
    view = pair_rep.reshape(chips, chunks, size, columns, channels)
    outs = pl.pallas_call(
        functools.partial(prepare_kernel, chips),
        out_shape=[jax.ShapeDtypeStruct((size, columns, channels), bf16)] * (chunks * chips),
        in_specs=vmem(2),
        out_specs=vmem(chunks * chips),
        name="prepare",
        compiler_params=room(kinds(pair_rep, pair_rep)),
        cost_estimate=estimate(rows * columns * channels * 12, 4 * pair_rep.size),
    )(view, norm_gain.reshape(1, channels))
    return [outs[piece * chips : (piece + 1) * chips] for piece in range(chunks)]


def assemble_kernel(chips, pieces, *refs):
    bias_refs, out_ref = refs[:pieces], refs[pieces]
    _, head_count, columns, share = bias_refs[0].shape
    length = out_ref.shape[1]
    count = chips * columns
    me = lax.axis_index("keys")
    here, core = me // cores, me % cores
    group = lax.axis_index("rows")
    place = lax.broadcasted_iota(jnp.int32, (share, length), 1)
    first = lax.broadcasted_iota(jnp.int32, (share, length), 0)
    side, block = place // count, place // columns % chips
    key = ((here ^ block) * cores + (core ^ side)) * columns + place % columns
    picks = [(key == (group ^ t) * share + first).astype(f32).astype(bf16) for t in range(pieces)]
    for h in range(head_count):
        for s in range(chips):
            total = jnp.zeros((columns, length), f32)
            for t in range(pieces):
                total += jnp.dot(bias_refs[t][s, h], picks[t], preferred_element_type=f32)
            start = h * count + s * columns
            out_ref[start : start + columns, :] = total


def assemble(bias_pieces):
    chips, head_count, columns, share = bias_pieces[0].shape
    pieces = len(bias_pieces)
    shape = (head_count * chips * columns, pieces * share)
    return pl.pallas_call(
        functools.partial(assemble_kernel, chips, pieces),
        out_shape=jax.ShapeDtypeStruct(shape, f32),
        in_specs=vmem(pieces),
        out_specs=pl.BlockSpec(memory_space=pltpu.VMEM),
        name="assemble",
        compiler_params=room(kinds(*bias_pieces) + [(shape, f32)]),
        cost_estimate=estimate(4 * shape[0] * shape[1] * shape[1], 6 * shape[0] * shape[1]),
    )(*bias_pieces)


def project_kernel(chips, head_size, *refs):
    own, refs = refs[:chips], refs[chips:]
    wq_ref, wk_ref, wv_ref, wg_ref, query_ref, gate_ref, key_ref, value_ref, asking_weights, held_weights = refs
    width = wq_ref.shape[1]
    asking_weights[:, :width] = wq_ref[...]
    asking_weights[:, width:] = wg_ref[...]
    held_weights[:, :width] = wk_ref[...]
    held_weights[:, width:] = wv_ref[...]
    scale = head_size ** (-0.5)

    def step(row, carry):
        rows = jnp.concatenate([own[s][row] for s in range(chips)], axis=0)
        asked = jnp.dot(rows, asking_weights[...], preferred_element_type=f32)
        query_ref[row] = (asked[:, :width] * scale).astype(bf16)
        gate_ref[row] = jax.nn.sigmoid(asked[:, width:])
        held = jnp.dot(rows, held_weights[...], preferred_element_type=f32).astype(bf16)
        key_ref[row] = held[:, :width]
        value_ref[row] = held[:, width:]
        return carry

    lax.fori_loop(0, own[0].shape[0], step, 0, unroll=2)


def project(own, weights, head_count):
    chips = len(own)
    rows, columns, channels = own[0].shape
    width = weights[0].shape[1]
    shape = (rows, chips * columns, width)
    return pl.pallas_call(
        functools.partial(project_kernel, chips, width // head_count),
        out_shape=[jax.ShapeDtypeStruct(shape, kind) for kind in (bf16, f32, bf16, bf16)],
        in_specs=vmem(chips + 4),
        out_specs=vmem(4),
        scratch_shapes=[pltpu.VMEM((channels, 2 * width), bf16)] * 2,
        name="project",
        compiler_params=room(kinds(*own) + [(shape, bf16)] * 5),
        cost_estimate=estimate(8 * rows * chips * columns * channels * width, 12 * rows * chips * columns * width),
    )(*own, *weights[:4])


def attend_kernel(chips, head_count, *refs):
    other, refs = refs[:chips], refs[chips:]
    query_ref, gate_ref, key_ref, value_ref, bias_ref, wk_ref, wv_ref, wo_ref = refs[:8]
    out_refs, refs = refs[8 : 8 + chips], refs[8 + chips :]
    keys, values, held_weights, logits_a, logits_b, highest_a, highest_b, powers_a, powers_b = refs
    rows, columns, channels = other[0].shape
    width = wk_ref.shape[1]
    count = chips * columns
    lanes = highest_a.shape[1]
    held_weights[:, :width] = wk_ref[...]
    held_weights[:, width:] = wv_ref[...]
    values[:, :, width:] = jnp.ones(values.shape[:2] + (width,), bf16)
    powers_b[...] = jnp.zeros_like(powers_b)

    def gather(row, carry):
        held = jnp.dot(
            jnp.concatenate([other[s][row] for s in range(chips)], axis=0),
            held_weights[...],
            preferred_element_type=f32,
        ).astype(bf16)
        keys[row, :count] = key_ref[row]
        keys[row, count:] = held[:, :width]
        values[row, :count, :width] = value_ref[row]
        values[row, count:, :width] = held[:, width:]
        return carry

    lax.fori_loop(0, rows, gather, 0, unroll=2)
    lane_head = lax.broadcasted_iota(jnp.int32, (count, width), 1) // (width // head_count)

    def score(row, logits, highest):
        query = query_ref[row]
        heads = [jnp.where(lane_head == h, query, jnp.zeros_like(query)) for h in range(head_count)]
        scores = lax.dot_general(
            jnp.concatenate(heads, axis=0),
            keys[row],
            (((1,), (1,)), ((), ())),
            preferred_element_type=f32,
        )
        scores = scores + bias_ref[...]
        logits[...] = scores
        highest[...] = jnp.broadcast_to(jnp.max(scores, axis=-1, keepdims=True), highest.shape)

    def weigh(logits, highest, powers):
        for start in range(0, logits.shape[1], lanes):
            part = slice(start, start + lanes)
            powers[:, part] = jnp.exp(logits[:, part] - highest[...]).astype(bf16)

    def finish(row, powers):
        both = jnp.dot(powers[...], values[row], preferred_element_type=f32)
        summed, total = both[:count, :width], both[:count, width:]
        for h in range(1, head_count):
            part = slice(h * count, (h + 1) * count)
            summed = jnp.where(lane_head == h, both[part, :width], summed)
            total = jnp.where(lane_head == h, both[part, width:], total)
        gated = (gate_ref[row] * (summed / total)).astype(bf16)
        update = jnp.dot(gated, wo_ref[...], preferred_element_type=f32).astype(bf16)
        for s in range(chips):
            out_refs[s][row] = update[s * columns : (s + 1) * columns]

    def pair(step, carry):
        row = 2 * step
        score(row + 1, logits_b, highest_b)
        weigh(logits_a, highest_a, powers_a)
        finish(jnp.maximum(row - 1, 0), powers_b)
        score(jnp.minimum(row + 2, rows - 1), logits_a, highest_a)
        weigh(logits_b, highest_b, powers_b)
        finish(row, powers_a)
        return carry

    score(0, logits_a, highest_a)
    lax.fori_loop(0, rows // 2, pair, 0)
    finish(rows - 1, powers_b)


def attend(other, projected, bias, weights, head_count):
    chips = len(other)
    rows, columns, channels = other[0].shape
    width = weights[0].shape[1]
    count, length = chips * columns, chips * cores * columns
    stacked = head_count * count
    flops = rows * (stacked * length * width * 6 + 2 * count * channels * width * 4)
    return pl.pallas_call(
        functools.partial(attend_kernel, chips, head_count),
        out_shape=[jax.ShapeDtypeStruct((rows, columns, channels), bf16)] * chips,
        in_specs=vmem(chips + 8),
        out_specs=vmem(chips),
        scratch_shapes=[
            pltpu.VMEM((rows, length, width), bf16),
            pltpu.VMEM((rows, length, 2 * width), bf16),
            pltpu.VMEM((channels, 2 * width), bf16),
        ]
        + [pltpu.VMEM((stacked, length), f32)] * 2
        + [pltpu.VMEM((stacked, 128), f32)] * 2
        + [pltpu.VMEM((stacked, length), bf16)] * 2,
        name="attend",
        compiler_params=room(
            kinds(*other, *other, *projected, bias)
            + [((rows, length, 3 * width), bf16), ((stacked, 2 * length + 256), f32), ((stacked, 2 * length), bf16)]
        ),
        cost_estimate=estimate(flops, 16 * rows * length * channels),
    )(*other, *projected, bias, weights[1], weights[2], weights[4])


def place_kernel(chips, *refs):
    here = lax.axis_index("keys") // cores
    out_ref = refs[-1]
    for piece in range(chunks):
        for s in range(chips):
            out_ref[here ^ s, piece] = refs[piece * chips + s][...]


def place(blocks, chips):
    size, columns, channels = blocks[0].shape
    out = pl.pallas_call(
        functools.partial(place_kernel, chips),
        out_shape=jax.ShapeDtypeStruct((chips, chunks, size, columns, channels), bf16),
        in_specs=vmem(len(blocks)),
        out_specs=pl.BlockSpec(memory_space=pltpu.VMEM),
        name="place",
        compiler_params=room(kinds(*blocks, *blocks)),
        cost_estimate=estimate(1000, 4 * size * columns * channels),
    )(*blocks)
    return out.reshape(chips * chunks * size, columns, channels)


def exchange_chips(block, s, chips):
    if s == 0:
        return block
    pairs = [(z * cores + c, (z ^ s) * cores + c) for z in range(chips) for c in range(cores)]
    return lax.ppermute(block, "keys", pairs)


def body(chips, groups, pair_rep, norm_gain, w_query, w_key, w_value, w_gate, w_out, pair_bias):
    head_count = pair_bias.shape[0]
    blocks = prepare(pair_rep, norm_gain, chips)
    mine = jnp.stack([exchange_chips(pair_bias, s, chips) for s in range(chips)])
    bias_pieces = [mine] + [
        lax.ppermute(mine, "rows", [(g, g ^ t) for g in range(groups)]) for t in range(1, groups)
    ]
    siblings = [(i, i ^ 1) for i in range(chips * cores)]
    weights = (w_query, w_key, w_value, w_gate, w_out)
    bias = assemble(bias_pieces)
    done = []
    for sent in blocks:
        own = [exchange_chips(sent[s], s, chips) for s in range(chips)]
        other = [lax.ppermute(block, "keys", siblings) for block in own]
        projected = project(own, weights, head_count)
        update = attend(other, projected, bias, weights, head_count)
        done += [exchange_chips(update[s], s, chips) for s in range(chips)]
    return place(done, chips)


def solution(mesh):
    placed = (P("rows", "keys", None), P(), P(), P(), P(), P(), P(), P(None, "keys", "rows"))
    chips = mesh.shape["keys"] // cores
    return jax.shard_map(
        functools.partial(body, chips, mesh.shape["rows"]),
        mesh=mesh,
        in_specs=placed,
        out_specs=P("rows", "keys", None),
        check_vma=False,
    )
```

```python
import functools
import math

import jax
import jax.numpy as jnp
from jax import lax
from jax.experimental import pallas as pl
from jax.experimental.pallas import tpu as pltpu
from jax.sharding import PartitionSpec as P

epsilon = 1e-05
cores = 2

f32 = jnp.float32
bf16 = jnp.bfloat16


def vmem(count):
    return [pl.BlockSpec(memory_space=pltpu.VMEM)] * count


def room(shapes, extra=4):
    size = sum(math.prod(s[:-1]) * max(s[-1], 128) * jnp.dtype(kind).itemsize for s, kind in shapes)
    return pltpu.CompilerParams(vmem_limit_bytes=min(size + extra * 2**20, 60 * 2**20))


def kinds(*arrays):
    return [(a.shape, a.dtype) for a in arrays]


def estimate(flops, size):
    return pl.CostEstimate(flops=flops, bytes_accessed=size, transcendentals=0)


def prepare_kernel(chips, x_ref, gain_ref, *out_refs):
    here = lax.axis_index("keys") // cores
    gain = gain_ref[...]
    for s in range(chips):
        values = x_ref[here ^ s].astype(f32)
        center = jnp.mean(values, axis=-1, keepdims=True)
        moved = values - center
        spread = jnp.mean(jnp.square(moved), axis=-1, keepdims=True)
        out_refs[s][...] = (moved * lax.rsqrt(spread + epsilon) * gain).astype(bf16)


def prepare(pair_rep, norm_gain, chips):
    rows, columns, channels = pair_rep.shape
    size = rows // chips
    return pl.pallas_call(
        functools.partial(prepare_kernel, chips),
        out_shape=[jax.ShapeDtypeStruct((size, columns, channels), bf16)] * chips,
        in_specs=vmem(2),
        out_specs=vmem(chips),
        name="prepare",
        compiler_params=room(kinds(pair_rep, pair_rep)),
        cost_estimate=estimate(rows * columns * channels * 12, 4 * pair_rep.size),
    )(pair_rep.reshape(chips, size, columns, channels), norm_gain.reshape(1, channels))


def stack_kernel(*refs):
    for s, ref in enumerate(refs[:-1]):
        refs[-1][s] = ref[...]


def stack(arrays):
    shape = jax.ShapeDtypeStruct((len(arrays),) + arrays[0].shape, arrays[0].dtype)
    return pl.pallas_call(
        stack_kernel,
        out_shape=shape,
        in_specs=vmem(len(arrays)),
        out_specs=pl.BlockSpec(memory_space=pltpu.VMEM),
        name="stack",
        compiler_params=room(kinds(shape, *arrays)),
        cost_estimate=estimate(arrays[0].size * 16, 4 * arrays[0].size * len(arrays)),
    )(*arrays)


def assemble_kernel(chips, pieces, *refs):
    bias_refs, out_ref = refs[:pieces], refs[pieces]
    _, head_count, columns, share = bias_refs[0].shape
    length = out_ref.shape[1]
    count = chips * columns
    me = lax.axis_index("keys")
    here, core = me // cores, me % cores
    group = lax.axis_index("rows")
    place = lax.broadcasted_iota(jnp.int32, (share, length), 1)
    first = lax.broadcasted_iota(jnp.int32, (share, length), 0)
    side, block = place // count, place // columns % chips
    key = ((here ^ block) * cores + (core ^ side)) * columns + place % columns
    picks = [(key == (group ^ t) * share + first).astype(f32).astype(bf16) for t in range(pieces)]
    for h in range(head_count):
        for s in range(chips):
            total = jnp.zeros((columns, length), f32)
            for t in range(pieces):
                total += jnp.dot(bias_refs[t][s, h], picks[t], preferred_element_type=f32)
            start = h * count + s * columns
            out_ref[start : start + columns, :] = total


def assemble(bias_pieces):
    chips, head_count, columns, share = bias_pieces[0].shape
    pieces = len(bias_pieces)
    shape = (head_count * chips * columns, pieces * share)
    return pl.pallas_call(
        functools.partial(assemble_kernel, chips, pieces),
        out_shape=jax.ShapeDtypeStruct(shape, f32),
        in_specs=vmem(pieces),
        out_specs=pl.BlockSpec(memory_space=pltpu.VMEM),
        name="assemble",
        compiler_params=room(kinds(*bias_pieces) + [(shape, f32)]),
        cost_estimate=estimate(4 * shape[0] * shape[1] * shape[1], 6 * shape[0] * shape[1]),
    )(*bias_pieces)


def hold_kernel(chips, *refs):
    own = refs[:chips]
    weights_ref, held_ref = refs[chips:]

    def step(row, carry):
        rows = jnp.concatenate([own[s][row] for s in range(chips)], axis=0)
        held_ref[row] = jnp.dot(rows, weights_ref[...], preferred_element_type=f32).astype(bf16)
        return carry

    lax.fori_loop(0, own[0].shape[0], step, 0, unroll=2)


def hold(own, weights):
    chips = len(own)
    rows, columns, channels = own[0].shape
    out = jax.ShapeDtypeStruct((rows, chips * columns, weights.shape[1]), bf16)
    return pl.pallas_call(
        functools.partial(hold_kernel, chips),
        out_shape=out,
        in_specs=vmem(chips + 1),
        out_specs=pl.BlockSpec(memory_space=pltpu.VMEM),
        name="hold",
        compiler_params=room(kinds(*own, weights, out)),
        cost_estimate=estimate(2 * out.size * channels, 4 * out.size),
    )(*own, weights)


def ask_kernel(chips, head_size, *refs):
    own, refs = refs[:chips], refs[chips:]
    weights_ref, refs = refs[0], refs[1:]
    query_refs, gate_refs = refs[:chips], refs[chips:]
    columns = own[0].shape[1]
    width = weights_ref.shape[1] // 2
    scale = head_size ** (-0.5)

    def step(row, carry):
        rows = jnp.concatenate([own[s][row] for s in range(chips)], axis=0)
        asked = jnp.dot(rows, weights_ref[...], preferred_element_type=f32)
        query = (asked[:, :width] * scale).astype(bf16)
        gate = jax.nn.sigmoid(asked[:, width:])
        for s in range(chips):
            query_refs[s][row] = query[s * columns : (s + 1) * columns]
            gate_refs[s][row] = gate[s * columns : (s + 1) * columns]
        return carry

    lax.fori_loop(0, own[0].shape[0], step, 0, unroll=2)


def ask(own, weights, head_count):
    chips = len(own)
    rows, columns, channels = own[0].shape
    width = weights.shape[1] // 2
    outs = [((rows, columns, width), kind) for kind in (bf16, f32) for _ in range(chips)]
    result = pl.pallas_call(
        functools.partial(ask_kernel, chips, width // head_count),
        out_shape=[jax.ShapeDtypeStruct(*out) for out in outs],
        in_specs=vmem(chips + 1),
        out_specs=vmem(2 * chips),
        name="ask",
        compiler_params=room(kinds(*own, weights) + outs),
        cost_estimate=estimate(4 * rows * chips * columns * channels * width, 8 * rows * chips * columns * width),
    )(*own, weights)
    return result[:chips], result[chips:]


def attend_kernel(slots, head_count, *refs):
    parts = len(slots)
    query_refs, refs = refs[:parts], refs[parts:]
    gate_refs, refs = refs[:parts], refs[parts:]
    held_ref, other_ref, bias_ref, weights_ref = refs[:4]
    out_refs, refs = refs[4 : 4 + parts], refs[4 + parts :]
    logits_a, logits_b, highest_a, highest_b, powers_a, powers_b, gated_ref = refs
    rows, columns, width = query_refs[0].shape
    length = held_ref.shape[1] * cores
    chips = held_ref.shape[1] // columns
    count = parts * columns
    lanes = highest_a.shape[1]
    ones = jnp.ones((length, width), bf16)
    lane_head = lax.broadcasted_iota(jnp.int32, (count, width), 1) // (width // head_count)

    def score(row, logits, highest):
        query = jnp.concatenate([ref[row] for ref in query_refs], axis=0)
        heads = [jnp.where(lane_head == h, query, jnp.zeros_like(query)) for h in range(head_count)]
        scores = lax.dot_general(
            jnp.concatenate(heads, axis=0),
            jnp.concatenate([held_ref[row, :, :width], other_ref[row, :, :width]], axis=0),
            (((1,), (1,)), ((), ())),
            preferred_element_type=f32,
        )
        for h in range(head_count):
            for i, s in enumerate(slots):
                part = pl.ds((h * parts + i) * columns, columns)
                start = (h * parts + i) * columns
                block = scores[start : start + columns] + bias_ref[pl.ds((h * chips + s) * columns, columns)]
                logits[part] = block
                highest[part] = jnp.broadcast_to(jnp.max(block, axis=-1, keepdims=True), (columns, lanes))

    def weigh(logits, highest, powers):
        for start in range(0, logits.shape[1], lanes):
            part = slice(start, start + lanes)
            powers[:, part] = jnp.exp(logits[:, part] - highest[...]).astype(bf16)

    def finish(row, powers):
        values = jnp.concatenate([held_ref[row, :, width:], other_ref[row, :, width:]], axis=0)
        both = jnp.dot(powers[...], jnp.concatenate([values, ones], axis=1), preferred_element_type=f32)
        summed, total = both[:count, :width], both[:count, width:]
        for h in range(1, head_count):
            part = slice(h * count, (h + 1) * count)
            summed = jnp.where(lane_head == h, both[part, :width], summed)
            total = jnp.where(lane_head == h, both[part, width:], total)
        gates = jnp.concatenate([ref[row] for ref in gate_refs], axis=0)
        gated = (gates * (summed / total)).astype(bf16)
        for i in range(parts):
            gated_ref[i, row] = gated[i * columns : (i + 1) * columns]

    def pair(step, carry):
        row = 2 * step
        score(row + 1, logits_b, highest_b)
        weigh(logits_a, highest_a, powers_a)
        if row > 0:
            finish(row - 1, powers_b)
        if row + 2 < rows:
            score(row + 2, logits_a, highest_a)
        weigh(logits_b, highest_b, powers_b)
        finish(row, powers_a)
        return carry

    score(0, logits_a, highest_a)
    for step in range(rows // 2):
        pair(step, 0)
    finish(rows - 1, powers_b)
    for i in range(parts):
        gated = gated_ref[i].reshape(rows * columns, width)
        update = jnp.dot(gated, weights_ref[...], preferred_element_type=f32).astype(bf16)
        out_refs[i][...] = update.reshape(rows, columns, width)


def attend(slots, queries, gates, held, other, bias, w_out, head_count):
    queries, gates = [queries[s] for s in slots], [gates[s] for s in slots]
    rows, columns, width = queries[0].shape
    length = held.shape[1] * cores
    stacked = head_count * len(slots) * columns
    out = jax.ShapeDtypeStruct((rows, columns, width), bf16)
    flops = rows * (stacked * length * width * 6 + 2 * len(slots) * columns * width * width)
    return pl.pallas_call(
        functools.partial(attend_kernel, slots, head_count),
        out_shape=[out] * len(slots),
        in_specs=vmem(2 * len(slots) + 4),
        out_specs=vmem(len(slots)),
        scratch_shapes=[pltpu.VMEM((stacked, length), f32)] * 2
        + [pltpu.VMEM((stacked, 128), f32)] * 2
        + [pltpu.VMEM((stacked, length), bf16)] * 2
        + [pltpu.VMEM((len(slots), rows, columns, width), bf16)],
        name="attend",
        compiler_params=room(
            kinds(*queries, *gates, held, other, bias, w_out, *([out] * len(slots)))
            + [((stacked, 2 * length + 256), f32), ((stacked, 2 * length), bf16)]
        ),
        cost_estimate=estimate(flops, 16 * rows * length * width),
    )(*queries, *gates, held, other, bias, w_out)


def place_kernel(chips, *refs):
    here = lax.axis_index("keys") // cores
    for s in range(chips):
        refs[-1][here ^ s] = refs[s][...]


def place(blocks, chips):
    size, columns, channels = blocks[0].shape
    out = pl.pallas_call(
        functools.partial(place_kernel, chips),
        out_shape=jax.ShapeDtypeStruct((chips, size, columns, channels), bf16),
        in_specs=vmem(len(blocks)),
        out_specs=pl.BlockSpec(memory_space=pltpu.VMEM),
        name="place",
        compiler_params=room(kinds(*blocks, *blocks)),
        cost_estimate=estimate(1000, 4 * size * columns * channels),
    )(*blocks)
    return out.reshape(chips * size, columns, channels)


def exchange_chips(block, s, chips):
    pairs = [(z * cores + c, (z ^ s) * cores + c) for z in range(chips) for c in range(cores)]
    return lax.ppermute(block, "keys", pairs)


def send(move, blocks):
    out = [blocks[0]]
    for s in range(1, len(blocks)):
        out.append(move(blocks[s], s))
    return out


def groups_of_slots(chips):
    half = chips // 2
    return [half, *range(1, half)], [*range(half + 1, chips), 0]


def body(chips, groups, pair_rep, norm_gain, w_query, w_key, w_value, w_gate, w_out, pair_bias):
    head_count = pair_bias.shape[0]
    along_z = lambda block, s: exchange_chips(block, s, chips)
    along_rows = lambda block, t: lax.ppermute(block, "rows", [(g, g ^ t) for g in range(groups)])
    siblings = [(i, i ^ 1) for i in range(chips * cores)]
    sent = prepare(pair_rep, norm_gain, chips)
    mine = stack(send(along_z, [pair_bias] * chips))
    bias_pieces = send(along_rows, [mine] * groups)
    own = send(along_z, sent)
    held = hold(own, jnp.concatenate([w_key, w_value], axis=1))
    other = lax.ppermute(held, "keys", siblings)
    queries, gates = ask(own, jnp.concatenate([w_query, w_gate], axis=1), head_count)
    bias = assemble(bias_pieces)
    update = [None] * chips
    for slots in groups_of_slots(chips):
        made = attend(slots, queries, gates, held, other, bias, w_out, head_count)
        for s, block in zip(slots, made):
            update[s] = block
    return place(send(along_z, update), chips)


def solution(mesh):
    placed = (P("rows", "keys", None), P(), P(), P(), P(), P(), P(), P(None, "keys", "rows"))
    chips, groups = mesh.shape["keys"] // cores, mesh.shape["rows"]
    return jax.shard_map(
        functools.partial(body, chips, groups),
        mesh=mesh,
        in_specs=placed,
        out_specs=P("rows", "keys", None),
        check_vma=False,
    )
```

```python
import functools
import math

import jax
import jax.numpy as jnp
from jax import lax
from jax.experimental import pallas as pl
from jax.experimental.pallas import tpu as pltpu
from jax.sharding import PartitionSpec as P

epsilon = 1e-05
cores = 2

f32 = jnp.float32
bf16 = jnp.bfloat16


def vmem(count):
    return [pl.BlockSpec(memory_space=pltpu.VMEM)] * count


def room(shapes, extra=4):
    size = sum(math.prod(s[:-1]) * max(s[-1], 128) * jnp.dtype(kind).itemsize for s, kind in shapes)
    return pltpu.CompilerParams(vmem_limit_bytes=min(size + extra * 2**20, 60 * 2**20))


def kinds(*arrays):
    return [(a.shape, a.dtype) for a in arrays]


def estimate(flops, size):
    return pl.CostEstimate(flops=flops, bytes_accessed=size, transcendentals=0)


def prepare_kernel(chips, x_ref, gain_ref, *out_refs):
    here = lax.axis_index("keys") // cores
    gain = gain_ref[...]
    for s in range(chips):
        values = x_ref[here ^ s].astype(f32)
        center = jnp.mean(values, axis=-1, keepdims=True)
        moved = values - center
        spread = jnp.mean(jnp.square(moved), axis=-1, keepdims=True)
        out_refs[s][...] = (moved * lax.rsqrt(spread + epsilon) * gain).astype(bf16)


def prepare(pair_rep, norm_gain, chips):
    rows, columns, channels = pair_rep.shape
    size = rows // chips
    return pl.pallas_call(
        functools.partial(prepare_kernel, chips),
        out_shape=[jax.ShapeDtypeStruct((size, columns, channels), bf16)] * chips,
        in_specs=vmem(2),
        out_specs=vmem(chips),
        name="prepare",
        compiler_params=room(kinds(pair_rep, pair_rep)),
        cost_estimate=estimate(rows * columns * channels * 8000, 4 * pair_rep.size),
    )(pair_rep.reshape(chips, size, columns, channels), norm_gain.reshape(1, channels))


def stack_kernel(*refs):
    for s, ref in enumerate(refs[:-1]):
        refs[-1][s] = ref[...]


def stack(blocks):
    shape = jax.ShapeDtypeStruct((len(blocks),) + blocks[0].shape, blocks[0].dtype)
    return pl.pallas_call(
        stack_kernel,
        out_shape=shape,
        in_specs=vmem(len(blocks)),
        out_specs=pl.BlockSpec(memory_space=pltpu.VMEM),
        name="stack",
        compiler_params=room(kinds(shape, *blocks)),
        cost_estimate=estimate(shape.size * 16, 4 * shape.size),
    )(*blocks)


def pick_kernel(pieces, chips, bias_ref, out_ref, packed_ref):
    heads = [bias_ref[h].astype(f32) for h in range(bias_ref.shape[0])]
    packed_ref[...] = jnp.concatenate(heads, axis=-1).astype(bf16)
    share, length = out_ref.shape[1:]
    columns = length // (chips * cores)
    count = chips * columns
    me = lax.axis_index("keys")
    here, core = me // cores, me % cores
    group = lax.axis_index("rows")
    place = lax.broadcasted_iota(jnp.int32, (1, length), 1)
    side, block = place // count, place // columns % chips
    key = ((here ^ block) * cores + (core ^ side)) * columns + place % columns
    first = lax.broadcasted_iota(jnp.int32, (share, length), 0)
    for t in range(pieces):
        out_ref[t] = (first == key - (group ^ t) * share).astype(f32).astype(bf16)


def pick(pieces, chips, pair_bias):
    head_count, columns, share = pair_bias.shape
    out = jax.ShapeDtypeStruct((pieces, share, pieces * share), bf16)
    packed = jax.ShapeDtypeStruct((columns, head_count * share), bf16)
    return pl.pallas_call(
        functools.partial(pick_kernel, pieces, chips),
        out_shape=[out, packed],
        in_specs=vmem(1),
        out_specs=vmem(2),
        name="pick",
        compiler_params=room(kinds(out, packed, pair_bias)),
        cost_estimate=estimate(out.size * 16000, 2 * out.size),
    )(pair_bias)


def assemble_kernel(head_count, *refs):
    bias_refs, pick_ref, out_ref = refs[:-2], refs[-2], refs[-1]
    chips, columns, lanes = bias_refs[0].shape
    share = lanes // head_count
    total = None
    for t, ref in enumerate(bias_refs):
        piece = ref[...].reshape(chips * columns, lanes).astype(f32)
        heads = [piece[:, h * share : (h + 1) * share] for h in range(head_count)]
        part = jnp.dot(jnp.concatenate(heads, axis=0).astype(bf16), pick_ref[t], preferred_element_type=f32)
        total = part if total is None else total + part
    out_ref[...] = total


def assemble(bias_pieces, picks, head_count):
    chips, columns, lanes = bias_pieces[0].shape
    shape = (head_count * chips * columns, len(bias_pieces) * lanes // head_count)
    return pl.pallas_call(
        functools.partial(assemble_kernel, head_count),
        out_shape=jax.ShapeDtypeStruct(shape, f32),
        in_specs=vmem(len(bias_pieces) + 1),
        out_specs=pl.BlockSpec(memory_space=pltpu.VMEM),
        name="assemble",
        compiler_params=room(kinds(*bias_pieces, picks) + [(shape, f32)] * 3),
        cost_estimate=estimate(2 * shape[0] * shape[1] * shape[1], 6 * shape[0] * shape[1]),
    )(*bias_pieces, picks)


def project(ref, weights):
    rows, columns, channels = ref.shape
    flat = ref[...].reshape(rows * columns, channels)
    return jnp.dot(flat, weights, preferred_element_type=f32).reshape(rows, columns, weights.shape[1])


def side_by_side(weights_ref, first):
    width = weights_ref.shape[1]
    parts = [weights_ref[i * width : (i + 1) * width] for i in (first, first + 1)]
    return jnp.concatenate(parts, axis=1)


def hold_kernel(chips, *refs):
    own = refs[:chips]
    weights_ref, held_ref = refs[chips:]
    weights = side_by_side(weights_ref, 0)
    columns = own[0].shape[1]
    for s in range(chips):
        held_ref[:, s * columns : (s + 1) * columns] = project(own[s], weights).astype(bf16)


def hold(own, weights):
    chips = len(own)
    rows, columns, channels = own[0].shape
    out = jax.ShapeDtypeStruct((rows, chips * columns, 2 * weights.shape[1]), bf16)
    return pl.pallas_call(
        functools.partial(hold_kernel, chips),
        out_shape=out,
        in_specs=vmem(chips + 1),
        out_specs=pl.BlockSpec(memory_space=pltpu.VMEM),
        name="hold",
        compiler_params=room(kinds(*own, weights, out, out)),
        cost_estimate=estimate(2 * out.size * channels, 4 * out.size),
    )(*own, weights)


def ask_kernel(chips, head_size, *refs):
    own, refs = refs[:chips], refs[chips:]
    weights_ref, refs = refs[0], refs[1:]
    query_refs, gate_refs = refs[:chips], refs[chips:]
    width = weights_ref.shape[1]
    weights = side_by_side(weights_ref, 2)
    scale = head_size ** (-0.5)
    for s in range(chips):
        asked = project(own[s], weights)
        query_refs[s][...] = (asked[:, :, :width] * scale).astype(bf16)
        gate_refs[s][...] = jax.nn.sigmoid(asked[:, :, width:])


def ask(own, weights, head_count):
    chips = len(own)
    rows, columns, channels = own[0].shape
    width = weights.shape[1]
    outs = [((rows, columns, width), kind) for kind in (bf16, f32) for _ in range(chips)]
    result = pl.pallas_call(
        functools.partial(ask_kernel, chips, width // head_count),
        out_shape=[jax.ShapeDtypeStruct(*out) for out in outs],
        in_specs=vmem(chips + 1),
        out_specs=vmem(2 * chips),
        name="ask",
        compiler_params=room(kinds(*own, weights) + outs + outs),
        cost_estimate=estimate(4 * rows * chips * columns * channels * width, 8 * rows * chips * columns * width),
    )(*own, weights)
    return result[:chips], result[chips:]


def attend_kernel(slots, held_parts, head_count, *refs):
    parts = len(slots)
    query_refs, refs = refs[:parts], refs[parts:]
    gate_refs, refs = refs[:parts], refs[parts:]
    held_refs, refs = refs[:held_parts], refs[held_parts:]
    bias_ref, weights_ref = refs[:2]
    out_refs, refs = refs[2 : 2 + parts], refs[2 + parts :]
    logits_a, logits_b, highest_a, highest_b, powers_a, powers_b, gated_ref = refs
    rows, columns, width = query_refs[0].shape
    length = sum(ref.shape[1] for ref in held_refs)
    chips = length // cores // columns
    count = parts * columns
    lanes = highest_a.shape[1]
    ones = jnp.ones((length, width), bf16)
    lane_head = lax.broadcasted_iota(jnp.int32, (count, width), 1) // (width // head_count)

    def score(row, logits, highest):
        query = jnp.concatenate([ref[row] for ref in query_refs], axis=0)
        heads = [jnp.where(lane_head == h, query, jnp.zeros_like(query)) for h in range(head_count)]
        scores = lax.dot_general(
            jnp.concatenate(heads, axis=0),
            jnp.concatenate([ref[row, :, :width] for ref in held_refs], axis=0),
            (((1,), (1,)), ((), ())),
            preferred_element_type=f32,
        )
        for h in range(head_count):
            for i, s in enumerate(slots):
                part = pl.ds((h * parts + i) * columns, columns)
                start = (h * parts + i) * columns
                block = scores[start : start + columns] + bias_ref[pl.ds((h * chips + s) * columns, columns)]
                logits[part] = block
                highest[part] = jnp.broadcast_to(jnp.max(block, axis=-1, keepdims=True), (columns, lanes))

    def weigh(logits, highest, powers):
        for start in range(0, logits.shape[1], lanes):
            part = slice(start, start + lanes)
            powers[:, part] = jnp.exp(logits[:, part] - highest[...]).astype(bf16)

    def finish(row, powers):
        values = jnp.concatenate([ref[row, :, width:] for ref in held_refs], axis=0)
        both = jnp.dot(powers[...], jnp.concatenate([values, ones], axis=1), preferred_element_type=f32)
        summed, total = both[:count, :width], both[:count, width:]
        for h in range(1, head_count):
            part = slice(h * count, (h + 1) * count)
            summed = jnp.where(lane_head == h, both[part, :width], summed)
            total = jnp.where(lane_head == h, both[part, width:], total)
        gates = jnp.concatenate([ref[row] for ref in gate_refs], axis=0)
        gated = (gates * (summed / total)).astype(bf16)
        for i in range(parts):
            gated_ref[i, row] = gated[i * columns : (i + 1) * columns]

    def pair(step, carry):
        row = 2 * step
        score(row + 1, logits_b, highest_b)
        weigh(logits_a, highest_a, powers_a)
        if row > 0:
            finish(row - 1, powers_b)
        if row + 2 < rows:
            score(row + 2, logits_a, highest_a)
        weigh(logits_b, highest_b, powers_b)
        finish(row, powers_a)
        return carry

    score(0, logits_a, highest_a)
    for step in range(rows // 2):
        pair(step, 0)
    finish(rows - 1, powers_b)
    for i in range(parts):
        gated = gated_ref[i].reshape(rows * columns, width)
        update = jnp.dot(gated, weights_ref[...], preferred_element_type=f32).astype(bf16)
        out_refs[i][...] = update.reshape(rows, columns, width)


def attend(slots, queries, gates, held, bias, w_out, head_count):
    queries, gates = [queries[s] for s in slots], [gates[s] for s in slots]
    rows, columns, width = queries[0].shape
    length = sum(part.shape[1] for part in held)
    stacked = head_count * len(slots) * columns
    out = jax.ShapeDtypeStruct((rows, columns, width), bf16)
    flops = rows * (stacked * length * width * 6 + 2 * len(slots) * columns * width * width)
    return pl.pallas_call(
        functools.partial(attend_kernel, slots, len(held), head_count),
        out_shape=[out] * len(slots),
        in_specs=vmem(2 * len(slots) + len(held) + 2),
        out_specs=vmem(len(slots)),
        scratch_shapes=[pltpu.VMEM((stacked, length), f32)] * 2
        + [pltpu.VMEM((stacked, 128), f32)] * 2
        + [pltpu.VMEM((stacked, length), bf16)] * 2
        + [pltpu.VMEM((len(slots), rows, columns, width), bf16)],
        name="attend",
        compiler_params=room(
            kinds(*queries, *gates, *held, bias, w_out, *([out] * len(slots)))
            + [((stacked, 2 * length + 256), f32), ((stacked, 2 * length), bf16)]
        ),
        cost_estimate=estimate(flops, 16 * rows * length * width),
    )(*queries, *gates, *held, bias, w_out)


def place_kernel(chips, *refs):
    here = lax.axis_index("keys") // cores
    out_ref, sems = refs[chips:]
    copies = [pltpu.make_async_copy(refs[s], out_ref.at[here ^ s], sems.at[s]) for s in range(chips)]
    for copy in copies:
        copy.start()
    for copy in copies:
        copy.wait()


def place(blocks, chips):
    size, columns, channels = blocks[0].shape
    out = pl.pallas_call(
        functools.partial(place_kernel, chips),
        out_shape=jax.ShapeDtypeStruct((chips, size, columns, channels), bf16),
        in_specs=vmem(len(blocks)),
        out_specs=pl.BlockSpec(memory_space=pltpu.HBM),
        scratch_shapes=[pltpu.SemaphoreType.DMA((chips,))],
        name="place",
        compiler_params=room(kinds(*blocks)),
        cost_estimate=estimate(1000, 4 * size * columns * channels),
    )(*blocks)
    return out.reshape(chips * size, columns, channels)


def exchange_chips(block, s, chips):
    pairs = [(z * cores + c, (z ^ s) * cores + c) for z in range(chips) for c in range(cores)]
    return lax.ppermute(block, "keys", pairs)


def send(move, blocks):
    out = [blocks[0]]
    for s in range(1, len(blocks)):
        out.append(move(blocks[s], s))
    return out


def groups_of_slots(chips):
    half = chips // 2
    return [half, *range(1, half)], [*range(half + 1, chips), 0]


def body(chips, groups, pair_rep, norm_gain, w_query, w_key, w_value, w_gate, w_out, pair_bias):
    head_count = pair_bias.shape[0]
    along_z = lambda block, s: exchange_chips(block, s, chips)
    along_rows = lambda block, t: lax.ppermute(block, "rows", [(g, g ^ t) for g in range(groups)])
    siblings = [(i, i ^ 1) for i in range(chips * cores)]
    picks, mine = pick(groups, chips, pair_bias)
    sent = prepare(pair_rep, norm_gain, chips)
    mine = stack(send(along_z, [mine] * chips))
    bias_pieces = send(along_rows, [mine] * groups)
    own = send(along_z, sent)
    weights = jnp.concatenate([w_key, w_value, w_query, w_gate], axis=0)
    cross = lambda block: lax.ppermute(block, "keys", siblings)
    early, late = own[: chips // 2], own[chips // 2 :]
    held = [hold(early, weights)]
    other = [cross(held[0])]
    queries, gates = ask(early, weights, head_count)
    crossed = []
    for block in late:
        crossed.append(cross(block))
    held.append(hold(late, weights))
    asked = ask(late, weights, head_count)
    queries, gates = queries + asked[0], gates + asked[1]
    other.append(hold(crossed, weights))
    bias = assemble(bias_pieces, picks, head_count)
    update = [None] * chips
    for slots in groups_of_slots(chips):
        made = attend(slots, queries, gates, held + other, bias, w_out, head_count)
        for s, block in zip(slots, made):
            update[s] = block
    return place(send(along_z, update), chips)


def solution(mesh):
    placed = (P("rows", "keys", None), P(), P(), P(), P(), P(), P(), P(None, "keys", "rows"))
    chips, groups = mesh.shape["keys"] // cores, mesh.shape["rows"]
    return jax.shard_map(
        functools.partial(body, chips, groups),
        mesh=mesh,
        in_specs=placed,
        out_specs=P("rows", "keys", None),
        check_vma=False,
    )
```
